512 devices in a mesh: delay: 32 (over y, z_lo), row: 4 (over x), col: 4 (over z_hi, core).
Axes of the slice: x: 4, y: 4, z: 16 (z_hi: 2, z_lo: 8; z = z_hi * 8 + z_lo), core: 2. Of those that a mesh axis runs over, the one named last changes fastest.
Arguments:
- excitation: bfloat16 [2, 3072, 128], P(None, 'row'), may hold values from -6 to 6
- delay_ops: bfloat16 [32, 3072, 3072], P('delay', 'row', 'col'), may hold values from -0.01953125 to 0.01953125
- inverse_op: bfloat16 [3072, 3072], P('col', 'row'), may hold values from -0.109375 to 0.109375
- history: bfloat16 [32, 3072, 128], P('delay', 'col'), may hold values from -6 to 6
Outputs:
- currents: bfloat16 [2, 3072, 128], P(None, 'col')
- final_history: bfloat16 [32, 3072, 128], P('delay', 'col')
The draws below stay inside these ranges and needn't reach their ends.
All inputs are finite; a program needn't handle non-finite values.
Results may differ from the reference program's by a relative error of at most 0.008.
Values may be sent and summed in bfloat16 or wider, within the bound.
A program may use at most 64 MiB of HBM per device.

```python
import jax
import jax.numpy as jnp
from jax import lax

N = 3072
EXC = 128
STEPS = 2
DELAYS = 32


def steps_of(rng, dims, split, smallest, top_value):
    factor_of = 1.0
    for dim, shards_of in split:
        steps = jax.random.uniform(jax.random.fold_in(jax.random.fold_in(rng, 6), dim), (shards_of,), jnp.float32, smallest / len(split), top_value / len(split))
        factor_of = factor_of * jnp.repeat(jnp.exp(steps), dims[dim] // shards_of).reshape((-1,) + (1,) * (len(dims) - 1 - dim))
    return factor_of


def gaussian(own_key, dims, width, most, shards=(), kind=jnp.bfloat16):
    factor_of = steps_of(own_key, dims, shards, -0.22, 0.18) if shards else 1.0
    entries = jax.random.normal(own_key, dims, jnp.float32) * width * factor_of
    return jnp.minimum(jnp.maximum(entries, -most), most).astype(kind)


def setup_inputs(seed: int = 0) -> dict:
    keys = jax.random.split(jax.random.key(seed), 5)
    excitation = gaussian(keys[0], (STEPS, N, EXC), 1.0, 6.0, ((1, 4),))
    delay_ops = gaussian(keys[1], (DELAYS, N, N), (N * DELAYS) ** -0.5, 0.01953125, ((0, 32), (1, 4), (2, 4)))
    inverse_op = gaussian(keys[2], (N, N), N ** -0.5, 0.109375, ((0, 4), (1, 4)))
    history = gaussian(keys[3], (DELAYS, N, EXC), 1.0, 6.0, ((0, 32), (1, 4)))
    return dict(excitation=excitation, delay_ops=delay_ops, inverse_op=inverse_op, history=history)


def reference(excitation, delay_ops, inverse_op, history):
    def advance(hist, incident):
        def add_delay(total, pair):
            operator, past = pair
            return total + jnp.dot(operator, past, preferred_element_type=jnp.float32), None

        start = jnp.zeros(hist.shape[1:], jnp.float32)
        retarded, unused = lax.scan(add_delay, start, (delay_ops, hist))
        rhs = (incident.astype(jnp.float32) - retarded).astype(jnp.bfloat16)
        current = jnp.dot(inverse_op, rhs, preferred_element_type=jnp.float32).astype(jnp.bfloat16)
        hist = jnp.concatenate([current[None], hist[:-1]], axis=0)
        return hist, current

    final_history, currents = lax.scan(advance, history, excitation)
    return currents, final_history
```

```python
import jax
import jax.numpy as jnp
from jax import lax
from jax.experimental import pallas as pl
from jax.experimental.pallas import tpu as pltpu
from jax.sharding import PartitionSpec as P

MESH = pl.DeviceIdType.MESH
F32, BF16 = jnp.float32, jnp.bfloat16
STEPS = 2
ROWS = 768
HALF = 384
EXC = 128
NY, NX, NZL, NZ = 4, 4, 8, 16
YE = EXC // NY
XE = YE // NX
NXY = NX * NY


def nt(a, b):
    return lax.dot_general(a, b, (((1,), (1,)), ((), ())), preferred_element_type=F32)


def kernel(exc_in, d_in, inv_in, h_in, cur_out, fin_out,
           exc, dop, inv, hist, hprev, hprev2,
           core_send, core_recv, own_half, y_send, y_recv, z_send, z_recv,
           d0_send, d0_recv, exc_t, rhs, c_own, x_send, x_recv, gath,
           load_sem, h_sem, core_sem, y_ssem, y_rsem, z_ssem, z_rsem,
           d0_ssem, d0_rsem, rhs_sem, x_ssem, x_rsem, b_ssem, b_rsem, g_ssem, g_rsem):
    d = lax.axis_index("delay")
    x = lax.axis_index("row")
    c = lax.axis_index("col")
    y, zl = d // NZL, d % NZL
    zh, k = c // 2, c % 2
    z = zh * NZL + zl
    xy = y * NX + x
    other = 1 - k
    hub = zl == 0
    cell0 = d == 0

    def at(yy, zz, xx, kk):
        return (yy * NZL + zz % NZL, xx, (zz // NZL) * 2 + kk)

    partner = at(y, z, x, other)

    loads = [
        pltpu.make_async_copy(h_in.at[0], hist, load_sem.at[0]),
        pltpu.make_async_copy(d_in.at[0], dop, load_sem.at[1]),
        pltpu.make_async_copy(exc_in, exc, load_sem.at[2]),
        pltpu.make_async_copy(inv_in, inv, load_sem.at[3]),
    ]
    for load in loads:
        load.start()

    barrier = pltpu.get_barrier_semaphore()

    def greet(device):
        pl.semaphore_signal(barrier, inc=1, device_id=device, device_id_type=MESH)

    greet(partner)
    for o in range(1, NXY):
        greet(at((y + o // NX) % NY, z, (x + o % NX) % NX, k))
    for o in range(1, NZ):
        greet(at(y, (z + o) % NZ, x, k))

    @pl.when(hub)
    def _():
        for o in range(1, NY):
            greet(at((y + o) % NY, (z + NZL) % NZ, x, k))

    for step, (low, high) in ((1, (1, NZL - 1)), (2, (2, NZL - 2))):
        @pl.when((zl >= high) & (y < NY - 1))
        def _():
            greet((d + step, x, c))

        @pl.when((zl < low) & (y > 0))
        def _():
            greet((d - step, x, c))

    def one(condition):
        return jnp.where(condition, 1, 0).astype(jnp.int32)

    up, down = y < NY - 1, y > 0
    peers = (
        1 + (NXY - 1) + (NZ - 1) + one(hub) * (NY - 1)
        + one((zl >= NZL - 1) & up) + one((zl < 1) & down)
        + one((zl >= NZL - 2) & up) + one((zl < 2) & down)
    )

    def remote(src, dst, ssem, rsem, device):
        return pltpu.make_async_remote_copy(
            src_ref=src, dst_ref=dst, send_sem=ssem, recv_sem=rsem,
            device_id=device, device_id_type=MESH,
        )

    def partial_sums(i, past):
        away = pl.ds(pl.multiple_of(other * HALF, HALF), HALF)
        mine = pl.ds(pl.multiple_of(k * HALF, HALF), HALF)
        core_send[i] = nt(past, dop[away, :]).astype(BF16)
        return mine

    def core_copy(i):
        return remote(core_send.at[i], core_recv.at[i], core_sem.at[i, 0], core_sem.at[i, 1], partner)

    def y_copy(s, o):
        peer = (y + o) % NY
        return remote(y_send.at[s, peer], y_recv.at[s, o - 1], y_ssem.at[s, o - 1],
                      y_rsem.at[s, o - 1], at(peer, z, x, k))

    def z_copy(s, hh):
        return remote(z_send.at[s], z_recv.at[s, z], z_ssem.at[s, hh], z_rsem.at[s, z],
                      at(y, hh * NZL, x, k))

    def y_stage(s):
        core_copy(s).wait_recv()
        total = own_half[s] + core_recv[s].astype(F32)
        y_send[s] = total.astype(BF16).reshape(NY, YE, HALF)
        for o in range(1, NY):
            y_copy(s, o).start()

    def z_stage(s):
        for o in range(1, NY):
            y_copy(s, o).wait_recv()
        total = y_send[s, y].astype(F32)
        for o in range(NY - 1):
            total = total + y_recv[s, o].astype(F32)
        z_send[s] = total.astype(BF16)
        for hh in range(2):
            @pl.when(z != hh * NZL)
            def _():
                z_copy(s, hh).start()

    h_copies = [
        remote(hist, hprev, h_sem.at[0], h_sem.at[1], (jnp.minimum(d + 1, 31), x, c)),
        remote(hist, hprev2, h_sem.at[2], h_sem.at[3], (jnp.minimum(d + 2, 31), x, c)),
    ]

    loads[0].wait()
    loads[1].wait()
    past = hist[...].astype(F32).T.astype(BF16)
    mine = partial_sums(0, past)
    pl.semaphore_wait(barrier, peers)
    core_copy(0).start()

    @pl.when(d < 31)
    def _():
        h_copies[0].start()

    own_half[0] = nt(past, dop[mine, :])
    y_stage(0)

    loads[2].wait()
    loads[3].wait()

    @pl.when(hub)
    def _():
        rows = pl.ds(pl.multiple_of(k * HALF, HALF), HALF)
        for s in range(STEPS):
            exc_t[s] = exc[s, rows, :].astype(F32).T.reshape(NY, YE, HALF)

    z_stage(0)

    @pl.when(d > 0)
    def _():
        h_copies[0].wait_recv()

    @pl.when(d == 0)
    def _():
        hprev[...] = jnp.zeros_like(hprev)

    past = hprev[...].astype(F32).T.astype(BF16)
    mine = partial_sums(1, past)
    core_copy(1).start()
    own_half[1] = nt(past, dop[mine, :])
    y_stage(1)
    z_stage(1)

    @pl.when(d < 30)
    def _():
        h_copies[1].start()

    def rhs_copy(s):
        return remote(rhs.at[s, k], rhs.at[s, k], rhs_sem.at[s, 0], rhs_sem.at[s, 1], partner)

    def rhs_arrival(s):
        return remote(rhs.at[s, other], rhs.at[s, other], rhs_sem.at[s, 0], rhs_sem.at[s, 1], partner)

    def x_copy(s, o):
        peer = (x + o) % NX
        return remote(x_send.at[s, peer], x_recv.at[s, o - 1], x_ssem.at[s, o - 1],
                      x_rsem.at[s, o - 1], at(y, z, peer, k))

    def b_copy(s, zz):
        return remote(gath.at[s, xy], gath.at[s, xy], b_ssem.at[s, zz - 1], b_rsem.at[s],
                      at(y, zh * NZL + zz, x, k))

    def g_copy(s, o):
        py, px = (y + o // NX) % NY, (x + o % NX) % NX
        return remote(gath.at[s, xy], gath.at[s, xy], g_ssem.at[s, o - 1], g_rsem.at[s, o - 1],
                      at(py, z, px, k))

    def g_arrival(s, o):
        py, px = (y + NY - o // NX) % NY, (x + NX - o % NX) % NX
        there = py * NX + px
        return remote(gath.at[s, there], gath.at[s, there], g_ssem.at[s, o - 1], g_rsem.at[s, o - 1],
                      at(py, z, px, k))

    def hub_step(s):
        total = exc_t[s, y] - z_send[s].astype(F32)
        for o in range(1, NZ):
            far = (z + o) % NZ
            remote(z_recv.at[s, far], z_recv.at[s, far], z_ssem.at[s, 0], z_rsem.at[s, far],
                   partner).wait_recv()
            total = total - z_recv[s, far].astype(F32)
        if s == 1:
            for hh in range(2):
                @pl.when(jnp.logical_not(cell0 & (zh == hh)))
                def _():
                    remote(d0_recv.at[hh], d0_recv.at[hh], d0_ssem.at[0], d0_rsem.at[hh],
                           partner).wait_recv()
            total = total - d0_recv[0].astype(F32) - d0_recv[1].astype(F32)
        rhs[s, k] = total.astype(BF16)
        rhs_copy(s).start()
        rhs_arrival(s).wait_recv()
        product = nt(rhs[s, 0], inv[:, :HALF]) + nt(rhs[s, 1], inv[:, HALF:])
        product = product.reshape(NX, XE, ROWS)
        c_own[...] = product
        x_send[s] = product.astype(BF16)
        for o in range(1, NX):
            x_copy(s, o).start()
        total = c_own[x]
        for o in range(1, NX):
            x_copy(s, o).wait_recv()
            total = total + x_recv[s, o - 1].astype(F32)
        gath[s, xy] = total.astype(BF16)
        if s == 1:
            for zz in range(NZL - 1, 0, -1):
                b_copy(s, zz).start()
        for o in range(1, NXY):
            g_copy(s, o).start()
        if s == 0:
            for zz in range(NZL - 1, 0, -1):
                b_copy(s, zz).start()

    def relay(s):
        b_copy(s, 1).wait_recv()
        for o in range(1, NXY):
            g_copy(s, o).start()

    def gathered(s):
        for o in range(1, NXY):
            g_arrival(s, o).wait_recv()

    def whole(s):
        return gath[s].astype(F32).reshape(EXC, ROWS)

    def d0_copy(o, hh):
        peer = (y + o) % NY
        return remote(d0_send.at[peer], d0_recv.at[zh], d0_ssem.at[o * 2 + hh], d0_rsem.at[zh],
                      at(peer, hh * NZL, x, k))

    @pl.when(hub)
    def _():
        hub_step(0)

    @pl.when(cell0)
    def _():
        gathered(0)
        mine = partial_sums(2, whole(0).astype(BF16))
        core_copy(2).start()
        own_half[0] = nt(whole(0).astype(BF16), dop[mine, :])
        core_copy(2).wait_recv()
        total = (own_half[0] + core_recv[2].astype(F32)).astype(BF16)
        d0_send[...] = total.reshape(NY, YE, HALF)
        d0_recv[zh] = d0_send[y]
        for hh in range(2):
            for o in range(NY):
                if o == 0:
                    @pl.when(zh != hh)
                    def _():
                        d0_copy(o, hh).start()
                else:
                    d0_copy(o, hh).start()

    @pl.when(hub)
    def _():
        hub_step(1)

    @pl.when(jnp.logical_not(hub))
    def _():
        relay(0)

    @pl.when(jnp.logical_not(cell0))
    def _():
        gathered(0)

    cur_out[0] = whole(0).T.astype(BF16)

    @pl.when(d == 1)
    def _():
        fin_out[0] = cur_out[0]

    @pl.when(d > 1)
    def _():
        h_copies[1].wait_recv()
        fin_out[0] = hprev2[...]

    @pl.when(jnp.logical_not(hub))
    def _():
        relay(1)

    gathered(1)
    cur_out[1] = whole(1).T.astype(BF16)

    @pl.when(d == 0)
    def _():
        fin_out[0] = cur_out[1]

    @pl.when(d < 31)
    def _():
        h_copies[0].wait_send()

    @pl.when(d < 30)
    def _():
        h_copies[1].wait_send()

    for s in range(STEPS):
        core_copy(s).wait_send()
        for o in range(1, NY):
            y_copy(s, o).wait_send()
        for hh in range(2):
            @pl.when(z != hh * NZL)
            def _():
                z_copy(s, hh).wait_send()
        for o in range(1, NXY):
            g_copy(s, o).wait_send()

    @pl.when(hub)
    def _():
        for s in range(STEPS):
            rhs_copy(s).wait_send()
            for o in range(1, NX):
                x_copy(s, o).wait_send()
            for zz in range(1, NZL):
                b_copy(s, zz).wait_send()

    @pl.when(cell0)
    def _():
        core_copy(2).wait_send()
        for hh in range(2):
            for o in range(NY):
                if o == 0:
                    @pl.when(zh != hh)
                    def _():
                        d0_copy(o, hh).wait_send()
                else:
                    d0_copy(o, hh).wait_send()


def on_device(excitation, delay_ops, inverse_op, history):
    vmem, dma = pltpu.VMEM, pltpu.SemaphoreType.DMA
    return pl.pallas_call(
        kernel,
        out_shape=(
            jax.ShapeDtypeStruct((STEPS, ROWS, EXC), BF16),
            jax.ShapeDtypeStruct((1, ROWS, EXC), BF16),
        ),
        in_specs=[pl.BlockSpec(memory_space=pl.ANY)] * 4,
        out_specs=(pl.BlockSpec(memory_space=pltpu.VMEM),) * 2,
        scratch_shapes=[
            vmem((STEPS, ROWS, EXC), BF16),
            vmem((ROWS, ROWS), BF16),
            vmem((ROWS, ROWS), BF16),
            vmem((ROWS, EXC), BF16),
            vmem((ROWS, EXC), BF16),
            vmem((ROWS, EXC), BF16),
            vmem((3, EXC, HALF), BF16),
            vmem((3, EXC, HALF), BF16),
            vmem((STEPS, EXC, HALF), F32),
            vmem((STEPS, NY, YE, HALF), BF16),
            vmem((STEPS, NY - 1, YE, HALF), BF16),
            vmem((STEPS, YE, HALF), BF16),
            vmem((STEPS, NZ, YE, HALF), BF16),
            vmem((NY, YE, HALF), BF16),
            vmem((2, YE, HALF), BF16),
            vmem((STEPS, NY, YE, HALF), F32),
            vmem((STEPS, 2, YE, HALF), BF16),
            vmem((NX, XE, ROWS), F32),
            vmem((STEPS, NX, XE, ROWS), BF16),
            vmem((STEPS, NX - 1, XE, ROWS), BF16),
            vmem((STEPS, NXY, XE, ROWS), BF16),
            dma((4,)),
            dma((4,)),
            dma((3, 2)),
            dma((STEPS, NY - 1)),
            dma((STEPS, NY - 1)),
            dma((STEPS, 2)),
            dma((STEPS, NZ)),
            dma((8,)),
            dma((2,)),
            dma((STEPS, 2)),
            dma((STEPS, NX - 1)),
            dma((STEPS, NX - 1)),
            dma((STEPS, NZL - 1)),
            dma((STEPS,)),
            dma((STEPS, NXY - 1)),
            dma((STEPS, NXY - 1)),
        ],
        compiler_params=pltpu.CompilerParams(collective_id=0, has_side_effects=True),
    )(excitation, delay_ops, inverse_op, history)


def solution(mesh):
    in_specs = (
        P(None, "row", None), P("delay", "row", "col"), P("col", "row"), P("delay", "col", None),
    )
    out_specs = (P(None, "col", None), P("delay", "col", None))
    return jax.shard_map(
        on_device, mesh=mesh, in_specs=in_specs, out_specs=out_specs, check_vma=False
    )
```

```python
import jax
import jax.numpy as jnp
from jax import lax
from jax.experimental import pallas as pl
from jax.experimental.pallas import tpu as pltpu
from jax.sharding import PartitionSpec as P

MESH = pl.DeviceIdType.MESH
F32, BF16 = jnp.float32, jnp.bfloat16
STEPS = 2
ROWS = 768
HALF = 384
EXC = 128
LANES = 128
NY, NX, NZL, NZ = 4, 4, 8, 16
YE = EXC // NY
XE = YE // NX
QUART = ROWS // NX
NXY = NX * NY


def nt(a, b):
    return lax.dot_general(a, b, (((1,), (1,)), ((), ())), preferred_element_type=F32)


def kernel(exc_in, d_in, inv_in, h_in, cur_out, fin_out,
           exc, dop, inv, hist, older,
           core_send, core_recv, own_half, y_send, y_recv, z_send, z_recv,
           d0_send, d0_recv, exc_t, rhs, c_own, x_send, x_recv, gath,
           load_sem, d_sem, h_sem, hx_ssem, hx_rsem, core_sem, y_ssem, y_rsem, z_ssem, z_rsem,
           d0_ssem, d0_rsem, rhs_sem, x_ssem, x_rsem, b_ssem, b_rsem, g_ssem, g_rsem):
    d = lax.axis_index("delay")
    x = lax.axis_index("row")
    c = lax.axis_index("col")
    y, zl = d // NZL, d % NZL
    zh, k = c // 2, c % 2
    z = zh * NZL + zl
    xy = y * NX + x
    other = 1 - k
    hub = zl == 0
    cell0 = d == 0

    def at(yy, zz, xx, kk):
        return (yy * NZL + zz % NZL, xx, (zz // NZL) * 2 + kk)

    partner = at(y, z, x, other)

    def d_load(i):
        part = pl.ds(pl.multiple_of(lax.rem(other * 3 + i, 6) * LANES, LANES), LANES)
        return pltpu.make_async_copy(d_in.at[0, part], dop.at[part], d_sem.at[i])

    loads = [
        pltpu.make_async_copy(h_in.at[0], hist, load_sem.at[0]),
        pltpu.make_async_copy(exc_in, exc, load_sem.at[1]),
        pltpu.make_async_copy(inv_in, inv, load_sem.at[2]),
    ]
    loads[0].start()
    for i in range(6):
        d_load(i).start()

    barrier = pltpu.get_barrier_semaphore()

    def greet(device):
        pl.semaphore_signal(barrier, inc=1, device_id=device, device_id_type=MESH)

    greet(partner)
    for o in range(1, NY):
        greet(at((y + o) % NY, z, x, k))
    for o in range(1, NX):
        greet(at(y, z, (x + o) % NX, k))

    @pl.when(hub)
    def _():
        for o in range(1, NZ):
            greet(at(y, (z + o) % NZ, x, k))

    @pl.when(d > 0)
    def _():
        greet((d - 1, x, c))

    @pl.when(d > 1)
    def _():
        greet((d - 2, x, c))

    def one(condition):
        return jnp.where(condition, 1, 0).astype(jnp.int32)

    peers = 1 + (NY - 1) + (NX - 1) + 2 - one(hub) + one(d < 31) + one(d < 30)

    def remote(src, dst, ssem, rsem, device):
        return pltpu.make_async_remote_copy(
            src_ref=src, dst_ref=dst, send_sem=ssem, recv_sem=rsem,
            device_id=device, device_id_type=MESH,
        )

    def partial_sums(i, past):
        away = pl.ds(pl.multiple_of(other * HALF, HALF), HALF)
        mine = pl.ds(pl.multiple_of(k * HALF, HALF), HALF)
        core_send[i] = nt(past, dop[away, :]).astype(BF16)
        return mine

    def core_copy(i):
        return remote(core_send.at[i], core_recv.at[i], core_sem.at[i, 0], core_sem.at[i, 1], partner)

    def y_copy(s, o):
        peer = (y + o) % NY
        return remote(y_send.at[s, peer], y_recv.at[s, o - 1], y_ssem.at[s, o - 1],
                      y_rsem.at[s, o - 1], at(peer, z, x, k))

    def z_copy(s, hh):
        return remote(z_send.at[s], z_recv.at[s, z], z_ssem.at[s, hh], z_rsem.at[s, z],
                      at(y, hh * NZL, x, k))

    def y_stage(s):
        core_copy(s).wait_recv()
        total = own_half[s] + core_recv[s].astype(F32)
        y_send[s] = total.astype(BF16).reshape(NY, YE, HALF)
        for o in range(1, NY):
            y_copy(s, o).start()

    def z_stage(s):
        for o in range(1, NY):
            y_copy(s, o).wait_recv()
        total = y_send[s, y].astype(F32)
        for o in range(NY - 1):
            total = total + y_recv[s, o].astype(F32)
        z_send[s] = total.astype(BF16)
        for hh in range(2):
            @pl.when(z != hh * NZL)
            def _():
                z_copy(s, hh).start()

    quarter = pl.ds(pl.multiple_of(x * QUART, QUART), QUART)

    def h_copy(i):
        return remote(hist.at[quarter], older.at[i, quarter], h_sem.at[i, 0], h_sem.at[i, 1],
                      (jnp.minimum(d + 1 + i, 31), x, c))

    def hx_copy(i, o):
        return remote(older.at[i, quarter], older.at[i, quarter], hx_ssem.at[i, o - 1],
                      hx_rsem.at[i, o - 1], at(y, z, (x + o) % NX, k))

    def hx_arrival(i, o):
        theirs = pl.ds(pl.multiple_of((x + NX - o) % NX * QUART, QUART), QUART)
        return remote(older.at[i, theirs], older.at[i, theirs], hx_ssem.at[i, o - 1],
                      hx_rsem.at[i, o - 1], partner)

    def h_pass(i):
        h_copy(i).wait_recv()
        for o in range(1, NX):
            hx_copy(i, o).start()

    def h_whole(i):
        for o in range(1, NX):
            hx_arrival(i, o).wait_recv()

    loads[0].wait()
    past = hist[...].astype(F32).T.astype(BF16)
    for i in range(3):
        d_load(i).wait()
    loads[1].start()
    loads[2].start()
    mine = partial_sums(0, past)
    pl.semaphore_wait(barrier, peers)
    core_copy(0).start()

    @pl.when(d < 31)
    def _():
        h_copy(0).start()

    for i in range(3, 6):
        d_load(i).wait()
    own_half[0] = nt(past, dop[mine, :])
    y_stage(0)
    loads[1].wait()
    loads[2].wait()

    @pl.when(hub)
    def _():
        rows = pl.ds(pl.multiple_of(k * HALF, HALF), HALF)
        for s in range(STEPS):
            exc_t[s] = exc[s, rows, :].astype(F32).T.reshape(NY, YE, HALF)

    z_stage(0)

    @pl.when(cell0)
    def _():
        y_send[1] = jnp.zeros_like(y_send[1])
        for o in range(1, NY):
            y_copy(1, o).start()

    def rhs_copy(s):
        return remote(rhs.at[s, k], rhs.at[s, k], rhs_sem.at[s, 0], rhs_sem.at[s, 1], partner)

    def rhs_arrival(s):
        return remote(rhs.at[s, other], rhs.at[s, other], rhs_sem.at[s, 0], rhs_sem.at[s, 1], partner)

    def x_copy(s, o):
        peer = (x + o) % NX
        return remote(x_send.at[s, peer], x_recv.at[s, o - 1], x_ssem.at[s, o - 1],
                      x_rsem.at[s, o - 1], at(y, z, peer, k))

    def b_copy(s, zz):
        return remote(gath.at[s, xy], gath.at[s, xy], b_ssem.at[s, zz - 1], b_rsem.at[s],
                      at(y, zh * NZL + zz, x, k))

    def g_copy(s, o):
        py, px = (y + o // NX) % NY, (x + o % NX) % NX
        return remote(gath.at[s, xy], gath.at[s, xy], g_ssem.at[s, o - 1], g_rsem.at[s, o - 1],
                      at(py, z, px, k))

    def g_arrival(s, o):
        py, px = (y + NY - o // NX) % NY, (x + NX - o % NX) % NX
        there = py * NX + px
        return remote(gath.at[s, there], gath.at[s, there], g_ssem.at[s, o - 1], g_rsem.at[s, o - 1],
                      at(py, z, px, k))

    def hub_step(s):
        total = exc_t[s, y] - z_send[s].astype(F32)
        for o in range(1, NZ):
            far = (z + o) % NZ
            remote(z_recv.at[s, far], z_recv.at[s, far], z_ssem.at[s, 0], z_rsem.at[s, far],
                   partner).wait_recv()
            total = total - z_recv[s, far].astype(F32)
        if s == 1:
            for hh in range(2):
                @pl.when(jnp.logical_not(cell0 & (zh == hh)))
                def _():
                    remote(d0_recv.at[hh], d0_recv.at[hh], d0_ssem.at[0], d0_rsem.at[hh],
                           partner).wait_recv()
            total = total - d0_recv[0].astype(F32) - d0_recv[1].astype(F32)
        rhs[s, k] = total.astype(BF16)
        rhs_copy(s).start()
        rhs_arrival(s).wait_recv()
        product = nt(rhs[s, 0], inv[:, :HALF]) + nt(rhs[s, 1], inv[:, HALF:])
        product = product.reshape(NX, XE, ROWS)
        c_own[...] = product
        x_send[s] = product.astype(BF16)
        for o in range(1, NX):
            x_copy(s, o).start()
        if s == 0:
            @pl.when(jnp.logical_not(cell0))
            def _():
                h_pass(0)
        total = c_own[x]
        for o in range(1, NX):
            x_copy(s, o).wait_recv()
            total = total + x_recv[s, o - 1].astype(F32)
        gath[s, xy] = total.astype(BF16)
        if s == 1:
            for zz in range(NZL - 1, 0, -1):
                b_copy(s, zz).start()
        for j in range(NY):
            oy = (NY - y + j) % NY
            for ox in range(NX):
                @pl.when((oy != 0) | (ox != 0))
                def _():
                    g_copy(s, oy * NX + ox).start()
        if s == 0:
            for zz in range(NZL - 1, 0, -1):
                b_copy(s, zz).start()

    def relay(s):
        b_copy(s, 1).wait_recv()
        for o in range(1, NXY):
            g_copy(s, o).start()

    def gathered(s):
        for o in range(1, NXY):
            g_arrival(s, o).wait_recv()

    def whole(s):
        return gath[s].astype(F32).reshape(EXC, ROWS)

    def d0_copy(o, hh):
        peer = (y + o) % NY
        return remote(d0_send.at[peer], d0_recv.at[zh], d0_ssem.at[o * 2 + hh], d0_rsem.at[zh],
                      at(peer, hh * NZL, x, k))

    @pl.when(hub)
    def _():
        hub_step(0)

    @pl.when(cell0)
    def _():
        gathered(0)
        mine = partial_sums(2, whole(0).astype(BF16))
        core_copy(2).start()
        own_half[0] = nt(whole(0).astype(BF16), dop[mine, :])
        core_copy(2).wait_recv()
        total = (own_half[0] + core_recv[2].astype(F32)).astype(BF16)
        d0_send[...] = total.reshape(NY, YE, HALF)
        d0_recv[zh] = d0_send[y]
        for o in (2, 1, 3, 0):
            d0_copy(o, 1 - zh).start()
        for o in range(1, NY):
            d0_copy(o, zh).start()

    @pl.when(jnp.logical_not(cell0))
    def _():
        @pl.when(jnp.logical_not(hub))
        def _():
            h_pass(0)

        h_whole(0)
        past = older[0].astype(F32).T.astype(BF16)
        mine = partial_sums(1, past)
        core_copy(1).start()
        own_half[1] = nt(past, dop[mine, :])
        y_stage(1)

    z_stage(1)

    @pl.when(d < 30)
    def _():
        h_copy(1).start()

    @pl.when(hub)
    def _():
        hub_step(1)

    @pl.when(jnp.logical_not(hub))
    def _():
        relay(0)

    @pl.when(jnp.logical_not(cell0))
    def _():
        gathered(0)

    @pl.when(d > 1)
    def _():
        h_pass(1)

    cur_out[0] = whole(0).T.astype(BF16)

    @pl.when(d == 1)
    def _():
        fin_out[0] = cur_out[0]

    @pl.when(d > 1)
    def _():
        h_whole(1)
        fin_out[0] = older[1]

    @pl.when(jnp.logical_not(hub))
    def _():
        relay(1)

    gathered(1)
    cur_out[1] = whole(1).T.astype(BF16)

    @pl.when(d == 0)
    def _():
        fin_out[0] = cur_out[1]

    for i in range(2):
        @pl.when(d < 31 - i)
        def _():
            h_copy(i).wait_send()

        @pl.when(d > i)
        def _():
            for o in range(1, NX):
                hx_copy(i, o).wait_send()

    core_copy(0).wait_send()

    @pl.when(jnp.logical_not(cell0))
    def _():
        core_copy(1).wait_send()

    for s in range(STEPS):
        for o in range(1, NY):
            y_copy(s, o).wait_send()
        for hh in range(2):
            @pl.when(z != hh * NZL)
            def _():
                z_copy(s, hh).wait_send()
        for o in range(1, NXY):
            g_copy(s, o).wait_send()

    @pl.when(hub)
    def _():
        for s in range(STEPS):
            rhs_copy(s).wait_send()
            for o in range(1, NX):
                x_copy(s, o).wait_send()
            for zz in range(1, NZL):
                b_copy(s, zz).wait_send()

    @pl.when(cell0)
    def _():
        core_copy(2).wait_send()
        for o in range(NY):
            d0_copy(o, 1 - zh).wait_send()
        for o in range(1, NY):
            d0_copy(o, zh).wait_send()


def store(cur, fin, cur_out, fin_out, sem):
    copies = [
        pltpu.make_async_copy(cur, cur_out, sem.at[0]),
        pltpu.make_async_copy(fin, fin_out, sem.at[1]),
    ]
    for copy in copies:
        copy.start()
    for copy in copies:
        copy.wait()


def on_device(excitation, delay_ops, inverse_op, history):
    vmem, dma = pltpu.VMEM, pltpu.SemaphoreType.DMA
    results = pl.pallas_call(
        kernel,
        out_shape=(vmem((STEPS, ROWS, EXC), BF16), vmem((1, ROWS, EXC), BF16)),
        in_specs=[pl.BlockSpec(memory_space=pl.ANY)] * 4,
        out_specs=(pl.BlockSpec(memory_space=pltpu.VMEM),) * 2,
        scratch_shapes=[
            vmem((STEPS, ROWS, EXC), BF16),
            vmem((ROWS, ROWS), BF16),
            vmem((ROWS, ROWS), BF16),
            vmem((ROWS, EXC), BF16),
            vmem((2, ROWS, EXC), BF16),
            vmem((3, EXC, HALF), BF16),
            vmem((3, EXC, HALF), BF16),
            vmem((STEPS, EXC, HALF), F32),
            vmem((STEPS, NY, YE, HALF), BF16),
            vmem((STEPS, NY - 1, YE, HALF), BF16),
            vmem((STEPS, YE, HALF), BF16),
            vmem((STEPS, NZ, YE, HALF), BF16),
            vmem((NY, YE, HALF), BF16),
            vmem((2, YE, HALF), BF16),
            vmem((STEPS, NY, YE, HALF), F32),
            vmem((STEPS, 2, YE, HALF), BF16),
            vmem((NX, XE, ROWS), F32),
            vmem((STEPS, NX, XE, ROWS), BF16),
            vmem((STEPS, NX - 1, XE, ROWS), BF16),
            vmem((STEPS, NXY, XE, ROWS), BF16),
            dma((3,)),
            dma((6,)),
            dma((2, 2)),
            dma((2, NX - 1)),
            dma((2, NX - 1)),
            dma((3, 2)),
            dma((STEPS, NY - 1)),
            dma((STEPS, NY - 1)),
            dma((STEPS, 2)),
            dma((STEPS, NZ)),
            dma((8,)),
            dma((2,)),
            dma((STEPS, 2)),
            dma((STEPS, NX - 1)),
            dma((STEPS, NX - 1)),
            dma((STEPS, NZL - 1)),
            dma((STEPS,)),
            dma((STEPS, NXY - 1)),
            dma((STEPS, NXY - 1)),
        ],
        compiler_params=pltpu.CompilerParams(collective_id=0, has_side_effects=True),
    )(excitation, delay_ops, inverse_op, history)
    return pl.pallas_call(
        store,
        out_shape=(
            jax.ShapeDtypeStruct((STEPS, ROWS, EXC), BF16),
            jax.ShapeDtypeStruct((1, ROWS, EXC), BF16),
        ),
        in_specs=[pl.BlockSpec(memory_space=pltpu.VMEM)] * 2,
        out_specs=(pl.BlockSpec(memory_space=pl.ANY),) * 2,
        scratch_shapes=[dma((2,))],
    )(*[pltpu.with_memory_space_constraint(r, pltpu.VMEM) for r in results])


def solution(mesh):
    in_specs = (
        P(None, "row", None), P("delay", "row", "col"), P("col", "row"), P("delay", "col", None),
    )
    out_specs = (P(None, "col", None), P("delay", "col", None))
    return jax.shard_map(
        on_device, mesh=mesh, in_specs=in_specs, out_specs=out_specs, check_vma=False
    )
```

```python
import jax
import jax.numpy as jnp
from jax import lax
from jax.experimental import pallas as pl
from jax.experimental.pallas import tpu as pltpu
from jax.sharding import PartitionSpec as P

MESH = pl.DeviceIdType.MESH
F32, BF16 = jnp.float32, jnp.bfloat16
STEPS = 2
ROWS = 768
HALF = 384
EXC = 128
LANES = 128
NY, NX, NZL, NZ = 4, 4, 8, 16
YE = EXC // NY
XE = YE // NX
QUART = ROWS // NX
NXY = NX * NY


def nt(a, b):
    return lax.dot_general(a, b, (((1,), (1,)), ((), ())), preferred_element_type=F32)


def kernel(exc_in, d_in, inv_in, h_in, cur_out, fin_out,
           exc, dop, inv, hist, older,
           core_send, core_recv, own_half, y_send, y_recv, z_send, z_recv,
           d0_send, d0_recv, exc_t, rhs, c_own, x_send, x_recv, gath,
           load_sem, d_sem, h_sem, hx_ssem, hx_rsem, core_sem, y_ssem, y_rsem, z_ssem, z_rsem,
           d0_ssem, d0_rsem, rhs_sem, x_ssem, x_rsem, b_ssem, b_rsem, g_ssem, g_rsem, far_sem):
    d = lax.axis_index("delay")
    x = lax.axis_index("row")
    c = lax.axis_index("col")
    y, zl = d // NZL, d % NZL
    zh, k = c // 2, c % 2
    z = zh * NZL + zl
    xy = y * NX + x
    other = 1 - k
    hub = zl == 0
    cell0 = d == 0

    def at(yy, zz, xx, kk):
        return (yy * NZL + zz % NZL, xx, (zz // NZL) * 2 + kk)

    partner = at(y, z, x, other)

    def d_load(i):
        part = pl.ds(pl.multiple_of(lax.rem(other * 3 + i, 6) * LANES, LANES), LANES)
        return pltpu.make_async_copy(d_in.at[0, part], dop.at[part], d_sem.at[i // 3])

    def d_half(i, which):
        part = pl.ds(pl.multiple_of(which * HALF, HALF), HALF)
        return pltpu.make_async_copy(d_in.at[0, part], dop.at[part], d_sem.at[i])

    loads = [
        pltpu.make_async_copy(h_in.at[0], hist, load_sem.at[0]),
        pltpu.make_async_copy(exc_in, exc, load_sem.at[1]),
        pltpu.make_async_copy(inv_in, inv, load_sem.at[2]),
    ]
    loads[0].start()
    for i in range(6):
        d_load(i).start()

    barrier = pltpu.get_barrier_semaphore()

    def greet(device):
        pl.semaphore_signal(barrier, inc=1, device_id=device, device_id_type=MESH)

    greet(partner)
    for o in range(1, NY):
        greet(at((y + o) % NY, z, x, k))
    for o in range(1, NX):
        greet(at(y, z, (x + o) % NX, k))

    @pl.when(hub)
    def _():
        for zz in range(NZL, NZ):
            @pl.when(z != zz)
            def _():
                greet(at(y, zz, x, k))

    @pl.when(z == 0)
    def _():
        for zz in range(1, NZL):
            greet(at(y, zz, x, k))

    @pl.when((zh == 0) & (zl > 0))
    def _():
        greet(at(y, NZL, x, k))

    @pl.when(d > 0)
    def _():
        greet((d - 1, x, c))

    @pl.when(d > 1)
    def _():
        greet((d - 2, x, c))

    def one(condition):
        return jnp.where(condition, 1, 0).astype(jnp.int32)

    peers = (
        1 + (NY - 1) + (NX - 1) + one(d < 31) + one(d < 30)
        + one(z > 0) + one(z > NZL) + one(z == NZL) * (NZL - 1)
    )

    def remote(src, dst, ssem, rsem, device):
        return pltpu.make_async_remote_copy(
            src_ref=src, dst_ref=dst, send_sem=ssem, recv_sem=rsem,
            device_id=device, device_id_type=MESH,
        )

    def partial_sums(i, past):
        away = pl.ds(pl.multiple_of(other * HALF, HALF), HALF)
        mine = pl.ds(pl.multiple_of(k * HALF, HALF), HALF)
        core_send[i] = nt(past, dop[away, :]).astype(BF16)
        return mine

    def core_copy(i):
        return remote(core_send.at[i], core_recv.at[i], core_sem.at[i, 0], core_sem.at[i, 1], partner)

    def y_copy(s, o):
        peer = (y + o) % NY
        return remote(y_send.at[s, peer], y_recv.at[s, o - 1], y_ssem.at[s], y_rsem.at[s],
                      at(peer, z, x, k))

    def all_of(ref, ssem, rsem):
        return remote(ref, ref, ssem, rsem, partner)

    def y_all(s):
        return all_of(y_recv.at[s], y_ssem.at[s], y_rsem.at[s])

    def z_copy(s, hh):
        return remote(z_send.at[s], z_recv.at[s, z], z_ssem.at[s, hh], z_rsem.at[s],
                      at(y, hh * NZL, x, k))

    def y_stage(s):
        core_copy(s).wait_recv()
        total = own_half[s] + core_recv[s].astype(F32)
        y_send[s] = total.astype(BF16).reshape(NY, YE, HALF)
        for o in range(1, NY):
            y_copy(s, o).start()

    def z_stage(s):
        y_all(s).wait_recv()
        total = y_send[s, y].astype(F32)
        for o in range(NY - 1):
            total = total + y_recv[s, o].astype(F32)
        z_send[s] = total.astype(BF16)
        for hh in range(2):
            if s == 0 and hh == 1:
                @pl.when(zh == 0)
                def _():
                    pl.semaphore_wait(far_sem, 1)

            @pl.when(z != hh * NZL)
            def _():
                z_copy(s, hh).start()

    quarter = pl.ds(pl.multiple_of(x * QUART, QUART), QUART)

    def h_copy(i):
        return remote(hist.at[quarter], older.at[i, quarter], h_sem.at[i, 0], h_sem.at[i, 1],
                      (jnp.minimum(d + 1 + i, 31), x, c))

    def hx_copy(i, o):
        return remote(older.at[i, quarter], older.at[i, quarter], hx_ssem.at[i], hx_rsem.at[i],
                      at(y, z, (x + o) % NX, k))

    def hx_all(i):
        return all_of(older.at[i, pl.ds(0, ROWS - QUART)], hx_ssem.at[i], hx_rsem.at[i])

    def h_pass(i):
        h_copy(i).wait_recv()
        for o in range(1, NX):
            hx_copy(i, o).start()

    def h_whole(i):
        hx_all(i).wait_recv()

    loads[0].wait()
    past = hist[...].astype(F32).T.astype(BF16)
    d_half(0, other).wait()
    loads[1].start()
    loads[2].start()
    mine = partial_sums(0, past)
    pl.semaphore_wait(barrier, peers)

    @pl.when(z == NZL)
    def _():
        for zz in range(NZL):
            pl.semaphore_signal(far_sem, inc=1, device_id=at(y, zz, x, k), device_id_type=MESH)

    core_copy(0).start()

    @pl.when(d < 31)
    def _():
        h_copy(0).start()

    d_half(1, k).wait()
    own_half[0] = nt(past, dop[mine, :])
    y_stage(0)
    loads[1].wait()
    loads[2].wait()

    @pl.when(hub)
    def _():
        rows = pl.ds(pl.multiple_of(k * HALF, HALF), HALF)
        for s in range(STEPS):
            exc_t[s] = exc[s, rows, :].astype(F32).T.reshape(NY, YE, HALF)

    z_stage(0)

    @pl.when(cell0)
    def _():
        y_send[1] = jnp.zeros_like(y_send[1])
        for o in range(1, NY):
            y_copy(1, o).start()

    def rhs_copy(s):
        return remote(rhs.at[s, k], rhs.at[s, k], rhs_sem.at[s, 0], rhs_sem.at[s, 1], partner)

    def rhs_arrival(s):
        return remote(rhs.at[s, other], rhs.at[s, other], rhs_sem.at[s, 0], rhs_sem.at[s, 1], partner)

    def x_copy(s, o):
        peer = (x + o) % NX
        return remote(x_send.at[s, peer], x_recv.at[s, o - 1], x_ssem.at[s], x_rsem.at[s],
                      at(y, z, peer, k))

    def x_all(s):
        return all_of(x_recv.at[s], x_ssem.at[s], x_rsem.at[s])

    def b_copy(s, zz):
        return remote(gath.at[s, xy], gath.at[s, xy], b_ssem.at[s], b_rsem.at[s],
                      at(y, zh * NZL + zz, x, k))

    def g_copy(s, o):
        py, px = (y + o // NX) % NY, (x + o % NX) % NX
        return remote(gath.at[s, xy], gath.at[s, xy], g_ssem.at[s], g_rsem.at[s],
                      at(py, z, px, k))

    def g_all(s):
        return all_of(gath.at[s, pl.ds(0, NXY - 1)], g_ssem.at[s], g_rsem.at[s])

    def hub_step(s):
        total = exc_t[s, y] - z_send[s].astype(F32)
        all_of(z_recv.at[s, pl.ds(0, NZ - 1)], z_ssem.at[s, 0], z_rsem.at[s]).wait_recv()
        for o in range(1, NZ):
            total = total - z_recv[s, (z + o) % NZ].astype(F32)
        if s == 1:
            @pl.when(cell0)
            def _():
                all_of(d0_recv.at[1 - zh], d0_ssem, d0_rsem).wait_recv()

            @pl.when(jnp.logical_not(cell0))
            def _():
                all_of(d0_recv, d0_ssem, d0_rsem).wait_recv()

            total = total - d0_recv[0].astype(F32) - d0_recv[1].astype(F32)
        rhs[s, k] = total.astype(BF16)
        rhs_copy(s).start()
        rhs_arrival(s).wait_recv()
        product = nt(rhs[s, 0], inv[:, :HALF]) + nt(rhs[s, 1], inv[:, HALF:])
        product = product.reshape(NX, XE, ROWS)
        c_own[...] = product
        x_send[s] = product.astype(BF16)
        for o in range(1, NX):
            x_copy(s, o).start()
        if s == 0:
            @pl.when(jnp.logical_not(cell0))
            def _():
                partial_of_next()
        total = c_own[x]
        x_all(s).wait_recv()
        for o in range(1, NX):
            total = total + x_recv[s, o - 1].astype(F32)
        gath[s, xy] = total.astype(BF16)
        if s == 1:
            for zz in range(1, NZL):
                b_copy(s, zz).start()
        for j in range(NY):
            oy = (NY - y + j) % NY
            for ox in range(NX):
                @pl.when((oy != 0) | (ox != 0))
                def _():
                    g_copy(s, oy * NX + ox).start()
        if s == 0:
            for zz in range(1, NZL):
                b_copy(s, zz).start()

    def relay(s):
        b_copy(s, 1).wait_recv()
        for o in range(1, NXY):
            g_copy(s, o).start()

    def gathered(s):
        g_all(s).wait_recv()

    def whole(s):
        return gath[s].astype(F32).reshape(EXC, ROWS)

    def d0_copy(o, hh):
        peer = (y + o) % NY
        return remote(d0_send.at[peer], d0_recv.at[zh], d0_ssem, d0_rsem,
                      at(peer, hh * NZL, x, k))

    def partial_of_next():
        h_whole(0)
        past = older[0].astype(F32).T.astype(BF16)
        mine = partial_sums(1, past)
        core_copy(1).start()
        own_half[1] = nt(past, dop[mine, :])

    @pl.when(jnp.logical_not(cell0))
    def _():
        h_pass(0)

        @pl.when(jnp.logical_not(hub))
        def _():
            partial_of_next()

    @pl.when(hub)
    def _():
        hub_step(0)

    @pl.when(cell0)
    def _():
        gathered(0)
        mine = partial_sums(2, whole(0).astype(BF16))
        core_copy(2).start()
        own_half[0] = nt(whole(0).astype(BF16), dop[mine, :])
        core_copy(2).wait_recv()
        total = (own_half[0] + core_recv[2].astype(F32)).astype(BF16)
        d0_send[...] = total.reshape(NY, YE, HALF)
        d0_recv[zh] = d0_send[y]
        for o in (2, 1, 3, 0):
            d0_copy(o, 1 - zh).start()
        for o in range(1, NY):
            d0_copy(o, zh).start()

    @pl.when(jnp.logical_not(cell0))
    def _():
        y_stage(1)

    z_stage(1)

    @pl.when(d < 30)
    def _():
        h_copy(1).start()

    @pl.when(hub)
    def _():
        hub_step(1)

    @pl.when(jnp.logical_not(hub))
    def _():
        relay(0)

    @pl.when(jnp.logical_not(cell0))
    def _():
        gathered(0)

    @pl.when(d > 1)
    def _():
        h_pass(1)

    cur_out[0] = whole(0).T.astype(BF16)

    @pl.when(d == 1)
    def _():
        fin_out[0] = cur_out[0]

    @pl.when(d > 1)
    def _():
        h_whole(1)
        fin_out[0] = older[1]

    @pl.when(jnp.logical_not(hub))
    def _():
        relay(1)

    gathered(1)
    cur_out[1] = whole(1).T.astype(BF16)

    @pl.when(d == 0)
    def _():
        fin_out[0] = cur_out[1]

    for i in range(2):
        @pl.when(d < 31 - i)
        def _():
            h_copy(i).wait_send()

        @pl.when(d > i)
        def _():
            hx_all(i).wait_send()

    core_copy(0).wait_send()

    @pl.when(jnp.logical_not(cell0))
    def _():
        core_copy(1).wait_send()

    for s in range(STEPS):
        y_all(s).wait_send()
        for hh in range(2):
            @pl.when(z != hh * NZL)
            def _():
                z_copy(s, hh).wait_send()
        g_all(s).wait_send()

    @pl.when(hub)
    def _():
        for s in range(STEPS):
            rhs_copy(s).wait_send()
            x_all(s).wait_send()
            all_of(gath.at[s, pl.ds(0, NZL - 1)], b_ssem.at[s], b_rsem.at[s]).wait_send()

    @pl.when(cell0)
    def _():
        core_copy(2).wait_send()
        all_of(z_recv.at[0, pl.ds(0, 2 * NY - 1)], d0_ssem, d0_rsem).wait_send()


def store(cur, fin, cur_out, fin_out, sem):
    copies = [
        pltpu.make_async_copy(cur, cur_out, sem.at[0]),
        pltpu.make_async_copy(fin, fin_out, sem.at[1]),
    ]
    for copy in copies:
        copy.start()
    for copy in copies:
        copy.wait()


def on_device(excitation, delay_ops, inverse_op, history):
    vmem, dma = pltpu.VMEM, pltpu.SemaphoreType.DMA
    results = pl.pallas_call(
        kernel,
        out_shape=(vmem((STEPS, ROWS, EXC), BF16), vmem((1, ROWS, EXC), BF16)),
        in_specs=[pl.BlockSpec(memory_space=pl.ANY)] * 4,
        out_specs=(pl.BlockSpec(memory_space=pltpu.VMEM),) * 2,
        scratch_shapes=[
            vmem((STEPS, ROWS, EXC), BF16),
            vmem((ROWS, ROWS), BF16),
            vmem((ROWS, ROWS), BF16),
            vmem((ROWS, EXC), BF16),
            vmem((2, ROWS, EXC), BF16),
            vmem((3, EXC, HALF), BF16),
            vmem((3, EXC, HALF), BF16),
            vmem((STEPS, EXC, HALF), F32),
            vmem((STEPS, NY, YE, HALF), BF16),
            vmem((STEPS, NY - 1, YE, HALF), BF16),
            vmem((STEPS, YE, HALF), BF16),
            vmem((STEPS, NZ, YE, HALF), BF16),
            vmem((NY, YE, HALF), BF16),
            vmem((2, YE, HALF), BF16),
            vmem((STEPS, NY, YE, HALF), F32),
            vmem((STEPS, 2, YE, HALF), BF16),
            vmem((NX, XE, ROWS), F32),
            vmem((STEPS, NX, XE, ROWS), BF16),
            vmem((STEPS, NX - 1, XE, ROWS), BF16),
            vmem((STEPS, NXY, XE, ROWS), BF16),
            dma((3,)),
            dma((2,)),
            dma((2, 2)),
            dma((2,)),
            dma((2,)),
            dma((3, 2)),
            dma((STEPS,)),
            dma((STEPS,)),
            dma((STEPS, 2)),
            dma((STEPS,)),
            dma,
            dma,
            dma((STEPS, 2)),
            dma((STEPS,)),
            dma((STEPS,)),
            dma((STEPS,)),
            dma((STEPS,)),
            dma((STEPS,)),
            dma((STEPS,)),
            pltpu.SemaphoreType.REGULAR,
        ],
        compiler_params=pltpu.CompilerParams(collective_id=0, has_side_effects=True),
    )(excitation, delay_ops, inverse_op, history)
    return pl.pallas_call(
        store,
        out_shape=(
            jax.ShapeDtypeStruct((STEPS, ROWS, EXC), BF16),
            jax.ShapeDtypeStruct((1, ROWS, EXC), BF16),
        ),
        in_specs=[pl.BlockSpec(memory_space=pltpu.VMEM)] * 2,
        out_specs=(pl.BlockSpec(memory_space=pl.ANY),) * 2,
        scratch_shapes=[dma((2,))],
    )(*[pltpu.with_memory_space_constraint(r, pltpu.VMEM) for r in results])


def solution(mesh):
    in_specs = (
        P(None, "row", None), P("delay", "row", "col"), P("col", "row"), P("delay", "col", None),
    )
    out_specs = (P(None, "col", None), P("delay", "col", None))
    return jax.shard_map(
        on_device, mesh=mesh, in_specs=in_specs, out_specs=out_specs, check_vma=False
    )
```

```python
import jax
import jax.numpy as jnp
from jax import lax
from jax.experimental import pallas as pl
from jax.experimental.pallas import tpu as pltpu
from jax.sharding import PartitionSpec as P

MESH = pl.DeviceIdType.MESH
F32, BF16 = jnp.float32, jnp.bfloat16
STEPS = 2
ROWS = 768
HALF = 384
EXC = 128
LANES = 128
NY, NX, NZL, NZ = 4, 4, 8, 16
YE = EXC // NY
XE = YE // NX
QUART = ROWS // NX
NXY = NX * NY


def nt(a, b):
    return lax.dot_general(a, b, (((1,), (1,)), ((), ())), preferred_element_type=F32)


def kernel(exc_in, d_in, inv_in, h_in, cur_out, fin_out,
           exc, dop, inv, inv_part, hist, older,
           core_send, core_recv, own_half, y_send, y_recv, z_send, z_recv,
           d0_send, d0_recv, exc_t, c_own, x_send, x_recv, gath,
           load_sem, d_sem, inv_sem, h_sem, hx_ssem, hx_rsem, core_sem, y_ssem, y_rsem, z_ssem, z_rsem,
           d0_ssem, d0_rsem, x_ssem, x_rsem, b_ssem, b_rsem, g_ssem, g_rsem, far_sem):
    d = lax.axis_index("delay")
    x = lax.axis_index("row")
    c = lax.axis_index("col")
    y, zl = d // NZL, d % NZL
    zh, k = c // 2, c % 2
    z = zh * NZL + zl
    xy = y * NX + x
    other = 1 - k
    hub = zl == 0
    cell0 = d == 0

    def at(yy, zz, xx, kk):
        return (yy * NZL + zz % NZL, xx, (zz // NZL) * 2 + kk)

    partner = at(y, z, x, other)

    def d_load(i):
        part = pl.ds(pl.multiple_of(lax.rem(other * 3 + i, 6) * LANES, LANES), LANES)
        return pltpu.make_async_copy(d_in.at[0, part], dop.at[part], d_sem.at[i // 3])

    def d_half(i, which):
        part = pl.ds(pl.multiple_of(which * HALF, HALF), HALF)
        return pltpu.make_async_copy(d_in.at[0, part], dop.at[part], d_sem.at[i])

    loads = [
        pltpu.make_async_copy(h_in.at[0], hist, load_sem.at[0]),
        pltpu.make_async_copy(exc_in, exc, load_sem.at[1]),
        pltpu.make_async_copy(inv_in.at[:, pl.ds(0, HALF)], inv.at[0], load_sem.at[2]),
        pltpu.make_async_copy(inv_in.at[:, pl.ds(HALF, HALF)], inv.at[1], load_sem.at[3]),
    ]
    loads[0].start()
    for i in range(6):
        d_load(i).start()

    barrier = pltpu.get_barrier_semaphore()

    def greet(device):
        pl.semaphore_signal(barrier, inc=1, device_id=device, device_id_type=MESH)

    greet(partner)
    for o in range(1, NY):
        greet(at((y + o) % NY, z, x, k))
    for o in range(1, NX):
        greet(at(y, z, (x + o) % NX, k))

    @pl.when(hub)
    def _():
        for zz in range(NZL, NZ):
            @pl.when(z != zz)
            def _():
                greet(at(y, zz, x, k))

    @pl.when(z == 0)
    def _():
        for zz in range(1, NZL):
            greet(at(y, zz, x, k))

    @pl.when((zh == 0) & (zl > 0))
    def _():
        greet(at(y, NZL, x, k))

    @pl.when(d > 0)
    def _():
        greet((d - 1, x, c))

    @pl.when(d > 1)
    def _():
        greet((d - 2, x, c))

    def one(condition):
        return jnp.where(condition, 1, 0).astype(jnp.int32)

    peers = (
        1 + (NY - 1) + (NX - 1) + one(d < 31) + one(d < 30)
        + one(z > 0) + one(z > NZL) + one(z == NZL) * (NZL - 1)
    )

    def remote(src, dst, ssem, rsem, device):
        return pltpu.make_async_remote_copy(
            src_ref=src, dst_ref=dst, send_sem=ssem, recv_sem=rsem,
            device_id=device, device_id_type=MESH,
        )

    def partial_sums(i, past):
        away = pl.ds(pl.multiple_of(other * HALF, HALF), HALF)
        mine = pl.ds(pl.multiple_of(k * HALF, HALF), HALF)
        core_send[i] = nt(past, dop[away, :]).astype(BF16)
        return mine

    def core_copy(i):
        return remote(core_send.at[i], core_recv.at[i], core_sem.at[i, 0], core_sem.at[i, 1], partner)

    def y_copy(s, o):
        peer = (y + o) % NY
        return remote(y_send.at[s, peer], y_recv.at[s, o - 1], y_ssem.at[s], y_rsem.at[s],
                      at(peer, z, x, k))

    def all_of(ref, ssem, rsem):
        return remote(ref, ref, ssem, rsem, partner)

    def y_all(s):
        return all_of(y_recv.at[s], y_ssem.at[s], y_rsem.at[s])

    def z_copy(s, hh):
        return remote(z_send.at[s], z_recv.at[s, z], z_ssem.at[s, hh], z_rsem.at[s],
                      at(y, hh * NZL, x, k))

    def y_stage(s):
        core_copy(s).wait_recv()
        total = own_half[s] + core_recv[s].astype(F32)
        y_send[s] = total.astype(BF16).reshape(NY, YE, HALF)
        for o in range(1, NY):
            y_copy(s, o).start()

    def z_stage(s):
        y_all(s).wait_recv()
        total = y_send[s, y].astype(F32)
        for o in range(NY - 1):
            total = total + y_recv[s, o].astype(F32)
        z_send[s] = total.astype(BF16)
        for hh in range(2):
            if s == 0 and hh == 1:
                @pl.when(zh == 0)
                def _():
                    pl.semaphore_wait(far_sem, 1)

            @pl.when(z != hh * NZL)
            def _():
                z_copy(s, hh).start()

    quarter = pl.ds(pl.multiple_of(x * QUART, QUART), QUART)

    def h_copy(i):
        return remote(hist.at[quarter], older.at[i, quarter], h_sem.at[i, 0], h_sem.at[i, 1],
                      (jnp.minimum(d + 1 + i, 31), x, c))

    def hx_copy(i, o):
        return remote(older.at[i, quarter], older.at[i, quarter], hx_ssem.at[i], hx_rsem.at[i],
                      at(y, z, (x + o) % NX, k))

    def hx_all(i):
        return all_of(older.at[i, pl.ds(0, ROWS - QUART)], hx_ssem.at[i], hx_rsem.at[i])

    def h_pass(i):
        h_copy(i).wait_recv()
        for o in range(1, NX):
            hx_copy(i, o).start()

    def h_whole(i):
        hx_all(i).wait_recv()

    loads[0].wait()
    past = hist[...].astype(F32).T.astype(BF16)
    d_half(0, other).wait()
    for load in loads[1:]:
        load.start()
    mine = partial_sums(0, past)
    pl.semaphore_wait(barrier, peers)

    @pl.when(z == NZL)
    def _():
        for zz in range(NZL):
            pl.semaphore_signal(far_sem, inc=1, device_id=at(y, zz, x, k), device_id_type=MESH)

    core_copy(0).start()

    @pl.when(d < 31)
    def _():
        h_copy(0).start()

    d_half(1, k).wait()
    own_half[0] = nt(past, dop[mine, :])
    y_stage(0)
    for load in loads[1:]:
        load.wait()

    inv_copy = remote(inv.at[other], inv_part, inv_sem.at[0], inv_sem.at[1], partner)

    @pl.when(hub)
    def _():
        inv_copy.start()
        rows = pl.ds(pl.multiple_of(k * HALF, HALF), HALF)
        for s in range(STEPS):
            exc_t[s] = exc[s, rows, :].astype(F32).T.reshape(NY, YE, HALF)

    z_stage(0)

    @pl.when(cell0)
    def _():
        y_send[1] = jnp.zeros_like(y_send[1])
        for o in range(1, NY):
            y_copy(1, o).start()

    def x_copy(s, o, kk):
        peer = (x + o) % NX
        return remote(x_send.at[s, kk, peer], x_recv.at[s, kk * NX + o - 1], x_ssem.at[s],
                      x_rsem.at[s], at(y, z, peer, k if kk == 0 else other))

    def x_all(s):
        return all_of(x_recv.at[s], x_ssem.at[s], x_rsem.at[s])

    def b_copy(s, zz):
        return remote(gath.at[s, xy], gath.at[s, xy], b_ssem.at[s], b_rsem.at[s],
                      at(y, zh * NZL + zz, x, k))

    def g_copy(s, o):
        py, px = (y + o // NX) % NY, (x + o % NX) % NX
        return remote(gath.at[s, xy], gath.at[s, xy], g_ssem.at[s], g_rsem.at[s],
                      at(py, z, px, k))

    def g_all(s):
        return all_of(gath.at[s, pl.ds(0, NXY - 1)], g_ssem.at[s], g_rsem.at[s])

    def hub_step(s):
        total = exc_t[s, y] - z_send[s].astype(F32)
        all_of(z_recv.at[s, pl.ds(0, NZ - 1)], z_ssem.at[s, 0], z_rsem.at[s]).wait_recv()
        for o in range(1, NZ):
            total = total - z_recv[s, (z + o) % NZ].astype(F32)
        if s == 1:
            @pl.when(cell0)
            def _():
                all_of(d0_recv.at[1 - zh], d0_ssem, d0_rsem).wait_recv()

            @pl.when(jnp.logical_not(cell0))
            def _():
                all_of(d0_recv, d0_ssem, d0_rsem).wait_recv()

            total = total - d0_recv[0].astype(F32) - d0_recv[1].astype(F32)
        rhs = total.astype(BF16)
        x_send[s, 1] = nt(rhs, inv_part[...]).reshape(NX, XE, ROWS).astype(BF16)
        for o in (2, 1, 3, 0):
            x_copy(s, o, 1).start()
        product = nt(rhs, inv[k]).reshape(NX, XE, ROWS)
        c_own[...] = product
        x_send[s, 0] = product.astype(BF16)
        for o in (2, 1, 3):
            x_copy(s, o, 0).start()
        if s == 0:
            @pl.when(jnp.logical_not(cell0))
            def _():
                partial_of_next()
                y_stage(1)
        total = c_own[x]
        x_all(s).wait_recv()
        for i in range(2 * NX - 1):
            total = total + x_recv[s, i].astype(F32)
        gath[s, xy] = total.astype(BF16)
        if s == 1:
            for zz in range(1, NZL):
                b_copy(s, zz).start()
        for j in range(NY):
            oy = (NY - y + j) % NY
            for ox in (2, 1, 3, 0):
                @pl.when((oy != 0) | (ox != 0))
                def _():
                    g_copy(s, oy * NX + ox).start()
        if s == 0:
            for zz in range(1, NZL):
                b_copy(s, zz).start()

    def relay(s):
        b_copy(s, 1).wait_recv()
        for o in sorted(range(1, NXY), key=lambda o: -min(o % NX, -o % NX) - min(o // NX, -(o // NX) % NY)):
            g_copy(s, o).start()

    def gathered(s):
        g_all(s).wait_recv()

    def whole(s):
        return gath[s].astype(F32).reshape(EXC, ROWS)

    def d0_copy(o, hh):
        peer = (y + o) % NY
        return remote(d0_send.at[peer], d0_recv.at[zh], d0_ssem, d0_rsem,
                      at(peer, hh * NZL, x, k))

    def partial_of_next():
        h_whole(0)
        past = older[0].astype(F32).T.astype(BF16)
        mine = partial_sums(1, past)
        core_copy(1).start()
        own_half[1] = nt(past, dop[mine, :])

    @pl.when(jnp.logical_not(cell0))
    def _():
        h_pass(0)

        @pl.when(jnp.logical_not(hub))
        def _():
            partial_of_next()
            y_stage(1)

    @pl.when(hub)
    def _():
        inv_copy.wait_recv()
        hub_step(0)

    z_stage(1)

    @pl.when(cell0)
    def _():
        gathered(0)
        mine = partial_sums(2, whole(0).astype(BF16))
        core_copy(2).start()
        own_half[0] = nt(whole(0).astype(BF16), dop[mine, :])
        core_copy(2).wait_recv()
        total = (own_half[0] + core_recv[2].astype(F32)).astype(BF16)
        d0_send[...] = total.reshape(NY, YE, HALF)
        d0_recv[zh] = d0_send[y]
        for o in (2, 1, 3, 0):
            d0_copy(o, 1 - zh).start()
        for o in range(1, NY):
            d0_copy(o, zh).start()

    @pl.when(d < 30)
    def _():
        h_copy(1).start()

    @pl.when(hub)
    def _():
        hub_step(1)

    @pl.when(jnp.logical_not(hub))
    def _():
        relay(0)

    @pl.when(jnp.logical_not(cell0))
    def _():
        gathered(0)

    @pl.when(d > 1)
    def _():
        h_pass(1)

    cur_out[0] = whole(0).T.astype(BF16)

    @pl.when(d == 1)
    def _():
        fin_out[0] = cur_out[0]

    @pl.when(d > 1)
    def _():
        h_whole(1)
        fin_out[0] = older[1]

    @pl.when(jnp.logical_not(hub))
    def _():
        relay(1)

    gathered(1)
    cur_out[1] = whole(1).T.astype(BF16)

    @pl.when(d == 0)
    def _():
        fin_out[0] = cur_out[1]

    for i in range(2):
        @pl.when(d < 31 - i)
        def _():
            h_copy(i).wait_send()

        @pl.when(d > i)
        def _():
            hx_all(i).wait_send()

    core_copy(0).wait_send()

    @pl.when(jnp.logical_not(cell0))
    def _():
        core_copy(1).wait_send()

    for s in range(STEPS):
        y_all(s).wait_send()
        for hh in range(2):
            @pl.when(z != hh * NZL)
            def _():
                z_copy(s, hh).wait_send()
        g_all(s).wait_send()

    @pl.when(hub)
    def _():
        inv_copy.wait_send()
        for s in range(STEPS):
            x_all(s).wait_send()
            all_of(gath.at[s, pl.ds(0, NZL - 1)], b_ssem.at[s], b_rsem.at[s]).wait_send()

    @pl.when(cell0)
    def _():
        core_copy(2).wait_send()
        all_of(z_recv.at[0, pl.ds(0, 2 * NY - 1)], d0_ssem, d0_rsem).wait_send()


def store(cur, fin, cur_out, fin_out, sem):
    copies = [
        pltpu.make_async_copy(cur, cur_out, sem.at[0]),
        pltpu.make_async_copy(fin, fin_out, sem.at[1]),
    ]
    for copy in copies:
        copy.start()
    for copy in copies:
        copy.wait()


def on_device(excitation, delay_ops, inverse_op, history):
    vmem, dma = pltpu.VMEM, pltpu.SemaphoreType.DMA
    results = pl.pallas_call(
        kernel,
        out_shape=(vmem((STEPS, ROWS, EXC), BF16), vmem((1, ROWS, EXC), BF16)),
        in_specs=[pl.BlockSpec(memory_space=pl.ANY)] * 4,
        out_specs=(pl.BlockSpec(memory_space=pltpu.VMEM),) * 2,
        scratch_shapes=[
            vmem((STEPS, ROWS, EXC), BF16),
            vmem((ROWS, ROWS), BF16),
            vmem((2, ROWS, HALF), BF16),
            vmem((ROWS, HALF), BF16),
            vmem((ROWS, EXC), BF16),
            vmem((2, ROWS, EXC), BF16),
            vmem((3, EXC, HALF), BF16),
            vmem((3, EXC, HALF), BF16),
            vmem((STEPS, EXC, HALF), F32),
            vmem((STEPS, NY, YE, HALF), BF16),
            vmem((STEPS, NY - 1, YE, HALF), BF16),
            vmem((STEPS, YE, HALF), BF16),
            vmem((STEPS, NZ, YE, HALF), BF16),
            vmem((NY, YE, HALF), BF16),
            vmem((2, YE, HALF), BF16),
            vmem((STEPS, NY, YE, HALF), F32),
            vmem((NX, XE, ROWS), F32),
            vmem((STEPS, 2, NX, XE, ROWS), BF16),
            vmem((STEPS, 2 * NX - 1, XE, ROWS), BF16),
            vmem((STEPS, NXY, XE, ROWS), BF16),
            dma((4,)),
            dma((2,)),
            dma((2,)),
            dma((2, 2)),
            dma((2,)),
            dma((2,)),
            dma((3, 2)),
            dma((STEPS,)),
            dma((STEPS,)),
            dma((STEPS, 2)),
            dma((STEPS,)),
            dma,
            dma,
            dma((STEPS,)),
            dma((STEPS,)),
            dma((STEPS,)),
            dma((STEPS,)),
            dma((STEPS,)),
            dma((STEPS,)),
            pltpu.SemaphoreType.REGULAR,
        ],
        compiler_params=pltpu.CompilerParams(collective_id=0, has_side_effects=True),
    )(excitation, delay_ops, inverse_op, history)
    return pl.pallas_call(
        store,
        out_shape=(
            jax.ShapeDtypeStruct((STEPS, ROWS, EXC), BF16),
            jax.ShapeDtypeStruct((1, ROWS, EXC), BF16),
        ),
        in_specs=[pl.BlockSpec(memory_space=pltpu.VMEM)] * 2,
        out_specs=(pl.BlockSpec(memory_space=pl.ANY),) * 2,
        scratch_shapes=[dma((2,))],
    )(*[pltpu.with_memory_space_constraint(r, pltpu.VMEM) for r in results])


def solution(mesh):
    in_specs = (
        P(None, "row", None), P("delay", "row", "col"), P("col", "row"), P("delay", "col", None),
    )
    out_specs = (P(None, "col", None), P("delay", "col", None))
    return jax.shard_map(
        on_device, mesh=mesh, in_specs=in_specs, out_specs=out_specs, check_vma=False
    )
```
